32 devices in a mesh: row: 4 (over y, x), col: 4 (over z), layer: 2 (over core).
Axes of the slice: x: 2, y: 2, z: 4, core: 2. Of those that a mesh axis runs over, the one named last changes fastest.
Arguments:
- hamiltonian: bfloat16 [4096, 4096], P('row', 'col'), as said below
- start_vectors: bfloat16 [256, 4096], P('row', ('col', 'layer')), may hold values from -6 to 6
- cut_low: float32 [1], replicated, may hold values from -1.6 to -1.2
- cut_high: float32 [1], replicated, may hold values from 2 to 2.4
Outputs:
- filtered: bfloat16 [256, 4096], P('row', ('col', 'layer'))
The draws below stay inside these ranges and needn't reach their ends.
Inputs may be any that keep to these rules, and one draw needn't show every extreme that they name: hamiltonian is exactly symmetric.
All inputs are finite; a program needn't handle non-finite values.
Results may differ from the reference program's by a relative error of at most 0.009.
Values may be sent and summed in bfloat16 or wider, within the bound.
No kernel may reach another device: no remote copies, remote signals or barrier semaphores. Data moves between devices by JAX's collectives and lax.ppermute only.
A program may use at most 64 MiB of HBM per device.

```python
import jax
import jax.numpy as jnp
from jax import lax

K = 256
NH = 4096


def draw_hamiltonian(key, part):
    entries = jax.random.normal(key, (NH, NH), jnp.float32)
    row_ids = lax.broadcasted_iota(jnp.int32, (NH, NH), 0)
    col_ids = lax.broadcasted_iota(jnp.int32, (NH, NH), 1)
    symmetric = jnp.where(row_ids <= col_ids, entries, entries.T)
    return (symmetric * NH ** (-0.5)).astype(jnp.bfloat16)


def levels(key, shape, cuts, smallest, largest):
    gain, own = 1.0, jax.random.fold_in(key, 6)
    for dim, shards_of in cuts:
        heights = jnp.exp(jax.random.uniform(jax.random.fold_in(own, dim), (shards_of,), jnp.float32, smallest / len(cuts), largest / len(cuts)))
        gain = gain * jnp.repeat(heights, shape[dim] // shards_of).reshape([-1 if axis == dim else 1 for axis in range(len(shape))])
    return gain


def gaussian(key, dims, deviation, bound, split=(), kind=jnp.bfloat16):
    level = levels(key, dims, split, -0.22, 0.18) if split else 1.0
    values = jax.random.normal(key, dims, jnp.float32) * deviation * level
    return jnp.minimum(jnp.maximum(values, -bound), bound).astype(kind)


def setup_inputs(seed: int = 0) -> dict:
    seeds = jax.random.split(jax.random.key(seed), 5)
    return {
        "hamiltonian": draw_hamiltonian(jax.random.fold_in(seeds[4], 71), 0),
        "start_vectors": gaussian(seeds[1], (K, NH), 1.0, 6.0, ((0, 4), (1, 8))),
        "cut_low": jnp.clip(jax.random.uniform(seeds[2], (1,), jnp.float32, -1.6, -1.2), -1.6, -1.2),
        "cut_high": jnp.clip(jax.random.uniform(seeds[3], (1,), jnp.float32, 2.0, 2.4), 2.0, 2.4),
    }


def apply_shifted(vectors, hamiltonian, centre, half_width):
    block_rows = min(1024, NH)
    count = NH // block_rows

    def one_block(block_index):
        first_row = (block_index * block_rows).astype(jnp.int32)
        rows = lax.dynamic_slice_in_dim(hamiltonian, first_row, block_rows, 0).astype(jnp.float32)
        row_ids = lax.broadcasted_iota(jnp.int32, (block_rows, NH), 0) + first_row
        col_ids = lax.broadcasted_iota(jnp.int32, (block_rows, NH), 1)
        diagonal_mask = (row_ids == col_ids).astype(jnp.float32)
        shifted = ((rows - centre * diagonal_mask) / half_width).astype(jnp.bfloat16)
        return lax.dot_general(vectors, shifted, (((1,), (1,)), ((), ())), preferred_element_type=jnp.float32)

    pieces = lax.map(one_block, jnp.arange(count, dtype=jnp.int32))
    return jnp.transpose(pieces, (1, 0, 2)).reshape(vectors.shape[0], NH)


def reference(hamiltonian, start_vectors, cut_low, cut_high):
    centre = (cut_low[0] + cut_high[0]) * 0.5
    half_width = (cut_high[0] - cut_low[0]) * 0.5
    first = apply_shifted(start_vectors, hamiltonian, centre, half_width).astype(jnp.bfloat16)
    second = (2.0 * apply_shifted(first, hamiltonian, centre, half_width) - start_vectors.astype(jnp.float32)).astype(jnp.bfloat16)
    third = (2.0 * apply_shifted(second, hamiltonian, centre, half_width) - first.astype(jnp.float32)).astype(jnp.bfloat16)
    filtered = (2.0 * apply_shifted(third, hamiltonian, centre, half_width) - second.astype(jnp.float32)).astype(jnp.bfloat16)
    return filtered
```

```python
import jax
import jax.numpy as jnp
from jax import lax
from jax.sharding import PartitionSpec as P


def make_shifted(block, first_row, first_col, centre, half_width):
    row_count, col_count = block.shape
    row_ids = lax.broadcasted_iota(jnp.int32, (row_count, col_count), 0) + first_row
    col_ids = lax.broadcasted_iota(jnp.int32, (row_count, col_count), 1) + first_col
    diagonal_mask = (row_ids == col_ids).astype(jnp.float32)
    return ((block.astype(jnp.float32) - centre * diagonal_mask) / half_width).astype(jnp.bfloat16)


def recurrence(begin, by_columns, by_rows):
    first = by_columns(begin).astype(jnp.bfloat16)
    second = (2.0 * by_rows(first) - begin.astype(jnp.float32)).astype(jnp.bfloat16)
    third = (2.0 * by_columns(second) - first.astype(jnp.float32)).astype(jnp.bfloat16)
    return (2.0 * by_rows(third) - second.astype(jnp.float32)).astype(jnp.bfloat16)


def partners(value, axis, count):
    pieces = value if isinstance(value, list) else [value] * count
    return [pieces[0]] + [
        lax.ppermute(pieces[step], axis, [(i, i ^ step) for i in range(count)]) for step in range(1, count)
    ]


def local_square(hamiltonian, start_vectors, cut_low, cut_high, count):
    centre = (cut_low[0] + cut_high[0]) * 0.5
    half_width = (cut_high[0] - cut_low[0]) * 0.5
    row, col, layer = lax.axis_index("row"), lax.axis_index("col"), lax.axis_index("layer")
    height, width = hamiltonian.shape
    whole = make_shifted(hamiltonian, row * height, col * width, centre, half_width)
    half = start_vectors.shape[0] // 2

    def panel_of(pieces):
        stacked = jnp.stack(pieces)
        return jnp.concatenate([lax.dynamic_index_in_dim(stacked, step ^ col, 0, False) for step in range(count)])

    def reduced(partial_value, axis):
        blocks = jnp.split(partial_value, count)
        sent = [blocks[0]] + [block.astype(jnp.bfloat16) for block in blocks[1:]]
        pieces = partners(sent, axis, count)
        return sum(piece.astype(jnp.float32) for piece in pieces)

    def by_columns(vectors):
        panel = panel_of(partners(vectors, "row", count))
        partial_value = lax.dot_general(
            panel, whole, (((1,), (1,)), ((), ())), preferred_element_type=jnp.float32
        )
        return reduced(partial_value, "col")

    def by_rows(vectors):
        panel = panel_of(partners(vectors, "col", count))
        return reduced(jnp.dot(panel, whole, preferred_element_type=jnp.float32), "row")

    swap = [(0, 1), (1, 0)]

    def halves(mine, other):
        return jnp.where(layer == 0, jnp.concatenate([mine, other], 1), jnp.concatenate([other, mine], 1))

    kept = lax.dynamic_slice_in_dim(start_vectors, layer * half, half, 0)
    given = lax.dynamic_slice_in_dim(start_vectors, (1 - layer) * half, half, 0)
    begin = halves(kept, lax.ppermute(given, "layer", swap))
    result = recurrence(begin, by_columns, by_rows)
    entries = width // 2
    kept = lax.dynamic_slice_in_dim(result, layer * entries, entries, 1)
    given = lax.dynamic_slice_in_dim(result, (1 - layer) * entries, entries, 1)
    other = lax.ppermute(given, "layer", swap)
    return jnp.where(layer == 0, jnp.concatenate([kept, other]), jnp.concatenate([other, kept]))


def local(hamiltonian, start_vectors, cut_low, cut_high):
    centre = (cut_low[0] + cut_high[0]) * 0.5
    half_width = (cut_high[0] - cut_low[0]) * 0.5
    row_count = hamiltonian.shape[0]
    first_row = lax.axis_index("row") * row_count
    width = hamiltonian.shape[1]
    whole = make_shifted(hamiltonian, first_row, lax.axis_index("col") * width, centre, half_width)

    def left_whole(panel):
        return lax.dot_general(
            panel, whole, (((1,), (1,)), ((), ())), preferred_element_type=jnp.float32
        )

    def right_whole(panel):
        return jnp.dot(panel, whole, preferred_element_type=jnp.float32)

    def by_columns(vectors):
        partial_value = left_whole(lax.all_gather(vectors, "row", axis=0, tiled=True))
        return lax.psum_scatter(partial_value, "col", scatter_dimension=0, tiled=True)

    def by_rows(vectors):
        partial_value = right_whole(lax.all_gather(vectors, "col", axis=0, tiled=True))
        return lax.psum_scatter(partial_value, "row", scatter_dimension=0, tiled=True)

    begin = lax.all_to_all(start_vectors, "layer", split_axis=0, concat_axis=1, tiled=True)
    result = recurrence(begin, by_columns, by_rows)
    return lax.all_to_all(result, "layer", split_axis=1, concat_axis=0, tiled=True)


def solution(mesh):
    rows, cols = mesh.shape["row"], mesh.shape["col"]
    square = rows == cols and rows & (rows - 1) == 0 and rows <= 8

    def body(*args):
        return local_square(*args, rows) if square else local(*args)

    return jax.shard_map(
        body,
        mesh=mesh,
        in_specs=(P("row", "col"), P("row", ("col", "layer")), P(), P()),
        out_specs=P("row", ("col", "layer")),
        check_vma=False,
    )
```

```python
import jax
import jax.numpy as jnp
from jax import lax
from jax.sharding import PartitionSpec as P


def make_shifted(block, first_row, first_col, centre, half_width):
    row_count, col_count = block.shape
    row_ids = lax.broadcasted_iota(jnp.int32, (row_count, col_count), 0) + first_row
    col_ids = lax.broadcasted_iota(jnp.int32, (row_count, col_count), 1) + first_col
    diagonal_mask = (row_ids == col_ids).astype(jnp.float32)
    return ((block.astype(jnp.float32) - centre * diagonal_mask) / half_width).astype(jnp.bfloat16)


def recurrence(begin, by_columns, by_rows):
    first = by_columns(begin).astype(jnp.bfloat16)
    second = (2.0 * by_rows(first) - begin.astype(jnp.float32)).astype(jnp.bfloat16)
    third = (2.0 * by_columns(second) - first.astype(jnp.float32)).astype(jnp.bfloat16)
    return (2.0 * by_rows(third) - second.astype(jnp.float32)).astype(jnp.bfloat16)


def scaled(block, first_row, first_col, centre, half_width):
    row_ids = lax.broadcasted_iota(jnp.int32, block.shape, 0) + first_row
    col_ids = lax.broadcasted_iota(jnp.int32, block.shape, 1) + first_col
    diagonal = jnp.where(row_ids == col_ids, centre, 0.0)
    return ((block.astype(jnp.float32) - diagonal) * (1.0 / half_width)).astype(jnp.bfloat16)


def total(pieces):
    return sum(piece.astype(jnp.float32) for piece in pieces)


def local_square(hamiltonian, start_vectors, cut_low, cut_high, count):
    row, col, layer = lax.axis_index("row"), lax.axis_index("col"), lax.axis_index("layer")
    height, width = hamiltonian.shape
    half = start_vectors.shape[0] // 2
    entries = width // 2
    swap = [(0, 1), (1, 0)]
    mixed = [0, 3, 1, 2] if count == 4 else list(range(count))
    unmixed = [mixed.index(step) for step in range(count)]
    mixed_col = sum(jnp.where(col == c, mixed[c], 0) for c in range(count))
    steps = list(range(1, count))
    last_steps = [1, 3, 0, 2] if count == 4 else list(range(count))

    def by_columns(panel):
        return lax.dot_general(panel, whole, (((1,), (1,)), ((), ())), preferred_element_type=jnp.float32)

    def by_rows(panel):
        return jnp.dot(panel, whole, preferred_element_type=jnp.float32)

    def picked(pieces, index):
        return lax.dynamic_index_in_dim(jnp.stack(pieces), index, 0, False)

    def partner(value, axis, step):
        return lax.ppermute(value, axis, [(i, i ^ step) for i in range(count)])

    def place(r, c, l):
        return (r * count + c) * 2 + l

    def crossed(value, step):
        pairs = []
        for r in range(count):
            for c in range(count):
                for l in range(2):
                    away = mixed[c] ^ mixed[step]
                    pairs.append((place(r, c, l), place(r ^ away, c, l if away else 1 - l)))
        return lax.ppermute(value, ("row", "col", "layer"), pairs)

    def product(value, axis_in, axis_out, times, table):
        got = {step: partner(value, axis_in, step) for step in steps}
        sent = [partner(times(got[step]).astype(jnp.bfloat16), axis_out, table[step]) for step in steps]
        own = lax.optimization_barrier(times(value))
        return [value] + [got[step] for step in steps], total([own] + sent)

    kept = lax.dynamic_slice_in_dim(start_vectors, layer * half, half, 0)
    other = lax.ppermute(start_vectors, "layer", swap)
    hamiltonian, kept, other = lax.optimization_barrier((hamiltonian, kept, other))
    centre = (cut_low[0] + cut_high[0]) * 0.5
    half_width = (cut_high[0] - cut_low[0]) * 0.5
    other = lax.dynamic_slice_in_dim(other, layer * half, half, 0)
    begin = jnp.where(layer == 0, jnp.concatenate([kept, other], 1), jnp.concatenate([other, kept], 1))
    gathered = [begin] + [partner(begin, "row", step) for step in steps]
    whole = scaled(hamiltonian, row * height, col * width, centre, half_width)

    panel = [picked(gathered, mixed_col ^ mixed[step]) for step in range(count)]
    values = jnp.split(by_columns(jnp.concatenate(panel)), count)
    sent = [partner(values[step].astype(jnp.bfloat16), "col", step) for step in steps]
    first = total([values[0]] + sent).astype(jnp.bfloat16)

    _, second = product(first, "col", "row", by_rows, mixed)
    second = (2.0 * second - panel[0].astype(jnp.float32)).astype(jnp.bfloat16)
    seconds, third = product(second, "row", "col", by_columns, unmixed)
    third = (2.0 * third - first.astype(jnp.float32)).astype(jnp.bfloat16)

    got = {step: partner(third, "col", step) for step in last_steps if step}
    got[0] = third
    result = []
    for step in last_steps:
        value = by_rows(got[step])
        back = crossed(value.astype(jnp.bfloat16), step)
        result.append(jnp.where(col == step, value, back.astype(jnp.float32)))
    result = 2.0 * sum(result) - picked(seconds, mixed_col).astype(jnp.float32)
    result = result.astype(jnp.bfloat16)

    kept = lax.dynamic_slice_in_dim(result, layer * entries, entries, 1)
    given = lax.dynamic_slice_in_dim(result, (1 - layer) * entries, entries, 1)
    other = lax.ppermute(given, "layer", swap)
    return jnp.where(layer == 0, jnp.concatenate([kept, other]), jnp.concatenate([other, kept]))


def local(hamiltonian, start_vectors, cut_low, cut_high):
    centre = (cut_low[0] + cut_high[0]) * 0.5
    half_width = (cut_high[0] - cut_low[0]) * 0.5
    row_count = hamiltonian.shape[0]
    first_row = lax.axis_index("row") * row_count
    width = hamiltonian.shape[1]
    whole = make_shifted(hamiltonian, first_row, lax.axis_index("col") * width, centre, half_width)

    def left_whole(panel):
        return lax.dot_general(
            panel, whole, (((1,), (1,)), ((), ())), preferred_element_type=jnp.float32
        )

    def right_whole(panel):
        return jnp.dot(panel, whole, preferred_element_type=jnp.float32)

    def by_columns(vectors):
        partial_value = left_whole(lax.all_gather(vectors, "row", axis=0, tiled=True))
        return lax.psum_scatter(partial_value, "col", scatter_dimension=0, tiled=True)

    def by_rows(vectors):
        partial_value = right_whole(lax.all_gather(vectors, "col", axis=0, tiled=True))
        return lax.psum_scatter(partial_value, "row", scatter_dimension=0, tiled=True)

    begin = lax.all_to_all(start_vectors, "layer", split_axis=0, concat_axis=1, tiled=True)
    result = recurrence(begin, by_columns, by_rows)
    return lax.all_to_all(result, "layer", split_axis=1, concat_axis=0, tiled=True)


def solution(mesh):
    rows, cols = mesh.shape["row"], mesh.shape["col"]
    square = rows == cols and rows & (rows - 1) == 0 and rows <= 8

    def body(*args):
        return local_square(*args, rows) if square else local(*args)

    return jax.shard_map(
        body,
        mesh=mesh,
        in_specs=(P("row", "col"), P("row", ("col", "layer")), P(), P()),
        out_specs=P("row", ("col", "layer")),
        check_vma=False,
    )
```

```python
import functools
import math

import jax
import jax.numpy as jnp
from jax import lax
from jax.experimental import pallas as pl
from jax.experimental.pallas import tpu as pltpu
from jax.sharding import PartitionSpec as P


MIXED = (0, 3, 1, 2)
SIDE = len(MIXED)


def make_shifted(block, first_row, first_col, centre, half_width):
    row_count, col_count = block.shape
    row_ids = lax.broadcasted_iota(jnp.int32, (row_count, col_count), 0) + first_row
    col_ids = lax.broadcasted_iota(jnp.int32, (row_count, col_count), 1) + first_col
    diagonal_mask = (row_ids == col_ids).astype(jnp.float32)
    return ((block.astype(jnp.float32) - centre * diagonal_mask) / half_width).astype(jnp.bfloat16)


def recurrence(begin, by_columns, by_rows):
    first = by_columns(begin).astype(jnp.bfloat16)
    second = (2.0 * by_rows(first) - begin.astype(jnp.float32)).astype(jnp.bfloat16)
    third = (2.0 * by_columns(second) - first.astype(jnp.float32)).astype(jnp.bfloat16)
    return (2.0 * by_rows(third) - second.astype(jnp.float32)).astype(jnp.bfloat16)


def shift_kernel(rows, block_ref, low_ref, high_ref, whole_ref, turned_ref):
    height, width = block_ref.shape
    low, high = low_ref[...], high_ref[...]
    centre = (low + high) * 0.5
    scale = 1.0 / ((high - low) * 0.5)
    offset = lax.axis_index("row") * height - lax.axis_index("col") * width
    gap = lax.broadcasted_iota(jnp.int32, (rows, width), 1) - lax.broadcasted_iota(jnp.int32, (rows, width), 0)
    for first in range(0, height, rows):
        entries = block_ref[pl.ds(first, rows), :].astype(jnp.float32)
        diagonal = jnp.where(gap == offset + first, centre, 0.0)
        shifted = ((entries - diagonal) * scale).astype(jnp.bfloat16)
        whole_ref[pl.ds(first, rows), :] = shifted
        turned_ref[:, pl.ds(first, rows)] = shifted.T


def both_shifted(block, cut_low, cut_high):
    height, width = block.shape
    vmem = pl.BlockSpec(memory_space=pltpu.VMEM)
    return pl.pallas_call(
        functools.partial(shift_kernel, math.gcd(height, 128)),
        out_shape=[jax.ShapeDtypeStruct(shape, block.dtype) for shape in ((height, width), (width, height))],
        in_specs=[vmem] * 3,
        out_specs=[vmem] * 2,
        cost_estimate=pl.CostEstimate(flops=4 * block.size, bytes_accessed=6 * block.size, transcendentals=0),
        compiler_params=pltpu.CompilerParams(vmem_limit_bytes=16 * block.size),
        name="shift",
    )(block, cut_low.reshape(1, 1), cut_high.reshape(1, 1))


def total(pieces):
    return sum(piece.astype(jnp.float32) for piece in pieces)


def local_direct(hamiltonian, start_vectors, cut_low, cut_high):
    col, layer = lax.axis_index("col"), lax.axis_index("layer")
    half, entries = start_vectors.shape[0] // 2, hamiltonian.shape[1] // 2
    swap = [(0, 1), (1, 0)]
    steps = range(1, SIDE)
    unmixed = [MIXED.index(step) for step in range(SIDE)]
    mixed_col = sum(jnp.where(col == c, MIXED[c], 0) for c in range(SIDE))

    def by_columns(panel):
        return jnp.dot(panel, turned, preferred_element_type=jnp.float32)

    def by_rows(panel):
        return jnp.dot(panel, whole, preferred_element_type=jnp.float32)

    def picked(pieces, index):
        return lax.dynamic_index_in_dim(jnp.stack(pieces), index, 0, False)

    def partner(value, axis, step):
        return lax.ppermute(value, axis, [(i, i ^ step) for i in range(SIDE)])

    def crossed(value, step):
        pairs = []
        for r in range(SIDE):
            for c in range(SIDE):
                for l in range(2):
                    away = MIXED[c] ^ MIXED[step]
                    pairs.append(((r * SIDE + c) * 2 + l, ((r ^ away) * SIDE + c) * 2 + (l if away else 1 - l)))
        return lax.ppermute(value, ("row", "col", "layer"), pairs)

    def product(value, axis_in, axis_out, times, table):
        got = [value] + [partner(value, axis_in, step) for step in steps]
        sent = [partner(times(got[step]).astype(jnp.bfloat16), axis_out, table[step]) for step in steps]
        own = lax.optimization_barrier(times(value))
        return got, total([own] + sent)

    kept = lax.dynamic_slice_in_dim(start_vectors, layer * half, half, 0)
    other = lax.ppermute(start_vectors, "layer", swap)
    kept, other = lax.optimization_barrier((kept, other))
    other = lax.dynamic_slice_in_dim(other, layer * half, half, 0)
    begin = jnp.where(layer == 0, jnp.concatenate([kept, other], 1), jnp.concatenate([other, kept], 1))
    begin, hamiltonian = lax.optimization_barrier((begin, hamiltonian))
    whole, turned = both_shifted(hamiltonian, cut_low, cut_high)

    gathered = [begin] + [partner(begin, "row", step) for step in steps]
    panel = [picked(gathered, mixed_col ^ MIXED[step]) for step in range(SIDE)]
    values = jnp.split(by_columns(jnp.concatenate(panel)), SIDE)
    sent = [partner(values[step].astype(jnp.bfloat16), "col", step) for step in steps]
    first = total([values[0]] + sent).astype(jnp.bfloat16)

    _, second = product(first, "col", "row", by_rows, MIXED)
    second = (2.0 * second - panel[0].astype(jnp.float32)).astype(jnp.bfloat16)
    seconds, third = product(second, "row", "col", by_columns, unmixed)
    third = (2.0 * third - first.astype(jnp.float32)).astype(jnp.bfloat16)

    gathered = [third] + [partner(third, "col", step) for step in steps]
    result = 0.0
    for step in range(SIDE):
        value = by_rows(gathered[step])
        back = crossed(value.astype(jnp.bfloat16), step)
        result += jnp.where(col == step, value, back.astype(jnp.float32))
    result = (2.0 * result - picked(seconds, mixed_col).astype(jnp.float32)).astype(jnp.bfloat16)

    kept = lax.dynamic_slice_in_dim(result, layer * entries, entries, 1)
    given = lax.dynamic_slice_in_dim(result, (1 - layer) * entries, entries, 1)
    other = lax.ppermute(given, "layer", swap)
    return jnp.where(layer == 0, jnp.concatenate([kept, other]), jnp.concatenate([other, kept]))


def local(hamiltonian, start_vectors, cut_low, cut_high):
    centre = (cut_low[0] + cut_high[0]) * 0.5
    half_width = (cut_high[0] - cut_low[0]) * 0.5
    row_count = hamiltonian.shape[0]
    first_row = lax.axis_index("row") * row_count
    width = hamiltonian.shape[1]
    whole = make_shifted(hamiltonian, first_row, lax.axis_index("col") * width, centre, half_width)

    def left_whole(panel):
        return lax.dot_general(
            panel, whole, (((1,), (1,)), ((), ())), preferred_element_type=jnp.float32
        )

    def right_whole(panel):
        return jnp.dot(panel, whole, preferred_element_type=jnp.float32)

    def by_columns(vectors):
        partial_value = left_whole(lax.all_gather(vectors, "row", axis=0, tiled=True))
        return lax.psum_scatter(partial_value, "col", scatter_dimension=0, tiled=True)

    def by_rows(vectors):
        partial_value = right_whole(lax.all_gather(vectors, "col", axis=0, tiled=True))
        return lax.psum_scatter(partial_value, "row", scatter_dimension=0, tiled=True)

    begin = lax.all_to_all(start_vectors, "layer", split_axis=0, concat_axis=1, tiled=True)
    result = recurrence(begin, by_columns, by_rows)
    return lax.all_to_all(result, "layer", split_axis=1, concat_axis=0, tiled=True)


def solution(mesh):
    direct = mesh.shape["row"] == SIDE and mesh.shape["col"] == SIDE and mesh.shape["layer"] == 2

    def body(*args):
        return local_direct(*args) if direct else local(*args)

    return jax.shard_map(
        body,
        mesh=mesh,
        in_specs=(P("row", "col"), P("row", ("col", "layer")), P(), P()),
        out_specs=P("row", ("col", "layer")),
        check_vma=False,
    )
```

```python
import functools
import math

import jax
import jax.numpy as jnp
from jax import lax
from jax.experimental import pallas as pl
from jax.experimental.pallas import tpu as pltpu
from jax.sharding import PartitionSpec as P


MIXED = (0, 3, 1, 2)
SIDE = len(MIXED)


def make_shifted(block, first_row, first_col, centre, half_width):
    row_count, col_count = block.shape
    row_ids = lax.broadcasted_iota(jnp.int32, (row_count, col_count), 0) + first_row
    col_ids = lax.broadcasted_iota(jnp.int32, (row_count, col_count), 1) + first_col
    diagonal_mask = (row_ids == col_ids).astype(jnp.float32)
    return ((block.astype(jnp.float32) - centre * diagonal_mask) / half_width).astype(jnp.bfloat16)


def recurrence(begin, by_columns, by_rows):
    first = by_columns(begin).astype(jnp.bfloat16)
    second = (2.0 * by_rows(first) - begin.astype(jnp.float32)).astype(jnp.bfloat16)
    third = (2.0 * by_columns(second) - first.astype(jnp.float32)).astype(jnp.bfloat16)
    return (2.0 * by_rows(third) - second.astype(jnp.float32)).astype(jnp.bfloat16)


def shift_kernel(rows, block_ref, low_ref, high_ref, whole_ref, turned_ref):
    height, width = block_ref.shape
    low, high = low_ref[...], high_ref[...]
    centre = (low + high) * 0.5
    scale = 1.0 / ((high - low) * 0.5)
    offset = lax.axis_index("row") * height - lax.axis_index("col") * width
    gap = lax.broadcasted_iota(jnp.int32, (rows, width), 1) - lax.broadcasted_iota(jnp.int32, (rows, width), 0)
    for first in range(0, height, rows):
        entries = block_ref[pl.ds(first, rows), :].astype(jnp.float32)
        diagonal = jnp.where(gap == offset + first, centre, 0.0)
        shifted = ((entries - diagonal) * scale).astype(jnp.bfloat16)
        whole_ref[pl.ds(first, rows), :] = shifted
        turned_ref[:, pl.ds(first, rows)] = shifted.T


def both_shifted(block, cut_low, cut_high):
    height, width = block.shape
    vmem = pl.BlockSpec(memory_space=pltpu.VMEM)
    return pl.pallas_call(
        functools.partial(shift_kernel, math.gcd(height, 128)),
        out_shape=[jax.ShapeDtypeStruct(shape, block.dtype) for shape in ((height, width), (width, height))],
        in_specs=[vmem] * 3,
        out_specs=[vmem] * 2,
        cost_estimate=pl.CostEstimate(flops=4 * block.size, bytes_accessed=6 * block.size, transcendentals=0),
        compiler_params=pltpu.CompilerParams(vmem_limit_bytes=16 * block.size),
        name="shift",
    )(block, cut_low.reshape(1, 1), cut_high.reshape(1, 1))


def total(pieces):
    return sum(piece.astype(jnp.float32) for piece in pieces)


def local_direct(hamiltonian, start_vectors, cut_low, cut_high):
    col, layer = lax.axis_index("col"), lax.axis_index("layer")
    half, entries = start_vectors.shape[0] // 2, hamiltonian.shape[1] // 2
    swap = [(0, 1), (1, 0)]
    steps = range(1, SIDE)
    unmixed = [MIXED.index(step) for step in range(SIDE)]
    mixed_col = sum(jnp.where(col == c, MIXED[c], 0) for c in range(SIDE))

    def by_columns(panel):
        return jnp.dot(panel, turned, preferred_element_type=jnp.float32)

    def by_rows(panel):
        return jnp.dot(panel, whole, preferred_element_type=jnp.float32)

    def picked(pieces, index):
        return lax.dynamic_index_in_dim(jnp.stack(pieces), index, 0, False)

    def partner(value, axis, step):
        return lax.ppermute(value, axis, [(i, i ^ step) for i in range(SIDE)])

    def crossed(value, step):
        pairs = []
        for r in range(SIDE):
            for c in range(SIDE):
                for l in range(2):
                    away = MIXED[c] ^ MIXED[step]
                    pairs.append(((r * SIDE + c) * 2 + l, ((r ^ away) * SIDE + c) * 2 + (l if away else 1 - l)))
        return lax.ppermute(value, ("row", "col", "layer"), pairs)

    def together(times, pieces):
        return jnp.split(times(jnp.concatenate(pieces)), len(pieces))

    def product(value, axis_in, axis_out, times, table, joined):
        got = [value] + [partner(value, axis_in, step) for step in steps]
        if joined:
            values = [times(got[1])] + together(times, got[2:])
        else:
            values = [times(got[step]) for step in steps]
        sent = [partner(values[step - 1].astype(jnp.bfloat16), axis_out, table[step]) for step in steps]
        own = lax.optimization_barrier(times(value))
        return got, total([own] + sent)

    kept = lax.dynamic_slice_in_dim(start_vectors, layer * half, half, 0)
    other = lax.ppermute(start_vectors, "layer", swap)
    kept, other = lax.optimization_barrier((kept, other))
    other = lax.dynamic_slice_in_dim(other, layer * half, half, 0)
    begin = jnp.where(layer == 0, jnp.concatenate([kept, other], 1), jnp.concatenate([other, kept], 1))
    begin, hamiltonian = lax.optimization_barrier((begin, hamiltonian))
    whole, turned = both_shifted(hamiltonian, cut_low, cut_high)

    gathered = [begin] + [partner(begin, "row", step) for step in steps]
    panel = [picked(gathered, mixed_col ^ MIXED[step]) for step in range(SIDE)]
    values = jnp.split(by_columns(jnp.concatenate(panel)), SIDE)
    sent = [partner(values[step].astype(jnp.bfloat16), "col", step) for step in steps]
    first = total([values[0]] + sent).astype(jnp.bfloat16)

    _, second = product(first, "col", "row", by_rows, MIXED, True)
    second = (2.0 * second - panel[0].astype(jnp.float32)).astype(jnp.bfloat16)
    seconds, third = product(second, "row", "col", by_columns, unmixed, False)
    third = (2.0 * third - first.astype(jnp.float32)).astype(jnp.bfloat16)

    gathered = [third] + [partner(third, "col", step) for step in steps]
    result = 0.0
    values = [by_rows(gathered[0]), by_rows(gathered[1])] + together(by_rows, gathered[2:])
    for step, value in enumerate(values):
        back = crossed(value.astype(jnp.bfloat16), step)
        result += jnp.where(col == step, value, back.astype(jnp.float32))
    result = (2.0 * result - picked(seconds, mixed_col).astype(jnp.float32)).astype(jnp.bfloat16)

    kept = lax.dynamic_slice_in_dim(result, layer * entries, entries, 1)
    given = lax.dynamic_slice_in_dim(result, (1 - layer) * entries, entries, 1)
    other = lax.ppermute(given, "layer", swap)
    return jnp.where(layer == 0, jnp.concatenate([kept, other]), jnp.concatenate([other, kept]))


def local(hamiltonian, start_vectors, cut_low, cut_high):
    centre = (cut_low[0] + cut_high[0]) * 0.5
    half_width = (cut_high[0] - cut_low[0]) * 0.5
    row_count = hamiltonian.shape[0]
    first_row = lax.axis_index("row") * row_count
    width = hamiltonian.shape[1]
    whole = make_shifted(hamiltonian, first_row, lax.axis_index("col") * width, centre, half_width)

    def left_whole(panel):
        return lax.dot_general(
            panel, whole, (((1,), (1,)), ((), ())), preferred_element_type=jnp.float32
        )

    def right_whole(panel):
        return jnp.dot(panel, whole, preferred_element_type=jnp.float32)

    def by_columns(vectors):
        partial_value = left_whole(lax.all_gather(vectors, "row", axis=0, tiled=True))
        return lax.psum_scatter(partial_value, "col", scatter_dimension=0, tiled=True)

    def by_rows(vectors):
        partial_value = right_whole(lax.all_gather(vectors, "col", axis=0, tiled=True))
        return lax.psum_scatter(partial_value, "row", scatter_dimension=0, tiled=True)

    begin = lax.all_to_all(start_vectors, "layer", split_axis=0, concat_axis=1, tiled=True)
    result = recurrence(begin, by_columns, by_rows)
    return lax.all_to_all(result, "layer", split_axis=1, concat_axis=0, tiled=True)


def solution(mesh):
    direct = mesh.shape["row"] == SIDE and mesh.shape["col"] == SIDE and mesh.shape["layer"] == 2

    def body(*args):
        return local_direct(*args) if direct else local(*args)

    return jax.shard_map(
        body,
        mesh=mesh,
        in_specs=(P("row", "col"), P("row", ("col", "layer")), P(), P()),
        out_specs=P("row", ("col", "layer")),
        check_vma=False,
    )
```
